8 devices in a mesh: data: 1 (over z), pp: 2 (over y), ep: 4 (over x, core).
Axes of the slice: x: 2, y: 2, z: 1, core: 2. Of those that a mesh axis runs over, the one named last changes fastest.
Arguments:
- expert_out: bfloat16 [2, 4, 128, 96, 4096], P('pp', 'data', 'ep')
- expert_ids: int32 [2, 4, 24, 64, 6], P('pp', 'data', 'ep')
- slot_ids: int32 [2, 4, 24, 64, 6], P('pp', 'data', 'ep')
- gate_weights: float32 [2, 4, 24, 64, 6], P('pp', 'data', 'ep')
- residual: bfloat16 [2, 4, 24, 64, 4096], P('pp', 'data', 'ep')
- norm_moe: float32 [2, 4096], P('pp')
- w_gate: bfloat16 [2, 4096, 2816], P('pp')
- w_up: bfloat16 [2, 4096, 2816], P('pp')
- w_down: bfloat16 [2, 2816, 4096], P('pp')
- norm_attn: float32 [2, 4096], P('pp')
- w_query: bfloat16 [2, 4096, 32, 128], P('pp')
- w_key: bfloat16 [2, 4096, 32, 128], P('pp')
- w_value: bfloat16 [2, 4096, 32, 128], P('pp')
- w_out: bfloat16 [2, 32, 128, 4096], P('pp')
Outputs:
- output: bfloat16 [2, 4, 24, 64, 4096], P('pp', 'data', 'ep')
All inputs are finite; a program needn't handle non-finite values.
Results may differ from the reference program's by a relative error of at most 0.0153595.
Values are sent between devices in bfloat16 or wider.
A program may use at most 1.25 GiB of HBM per device.

```python
import math
import jax
import jax.numpy as jnp
from jax import lax

STAGES = 2
EP_SIZE = 4
MICRO_BATCHES = 4
SEQ_DEV = 6
SEQ_LEN = 64
D_MODEL = 4096
NUM_HEADS = 32
HEAD_DIM = 128
EXPERTS = 128
TOP_K = 6
FF_SHARED = 2816
CAP_SLOTS = 24

SEQS = EP_SIZE * SEQ_DEV
TOK_DEV = SEQ_DEV * SEQ_LEN
TOKENS = SEQS * SEQ_LEN
SLOTS = EP_SIZE * CAP_SLOTS
HEADS_WIDTH = NUM_HEADS * HEAD_DIM
SCORE_SCALE = 1.0 / math.sqrt(HEAD_DIM)
EPSILON = 1e-6


def route_group(group_args):
    group_key, hot_draw = group_args
    hot_rank = jnp.argsort(jnp.argsort(hot_draw * EXPERTS + jnp.arange(EXPERTS)))
    lead_mask = (jnp.arange(TOK_DEV) <= CAP_SLOTS).astype(jnp.int32)[:, None]
    hot_bias = jnp.where(hot_rank < max(1, TOP_K // 4), 1024, 0) + jnp.where(hot_rank == 0, 8192, 0) * lead_mask
    noise_draw = jax.random.randint(group_key, (EP_SIZE, TOK_DEV, EXPERTS), 0, 4096)
    scores = (noise_draw + hot_bias) * EXPERTS + jnp.arange(EXPERTS)
    top_vals, expert_ids = lax.top_k(scores, TOP_K)
    choice_count = TOK_DEV * TOP_K
    flat_ids = expert_ids.reshape(EP_SIZE, choice_count)
    position = jnp.arange(choice_count)
    sort_order = jnp.argsort(flat_ids * choice_count + position, axis=-1)
    sorted_ids = jnp.take_along_axis(flat_ids, sort_order, axis=-1)
    is_start = jnp.concatenate([jnp.ones((EP_SIZE, 1), jnp.bool_), sorted_ids[:, 1:] != sorted_ids[:, :-1]], axis=1)
    start_pos = lax.cummax(jnp.where(is_start, position, 0), axis=1)
    slot_rank = jnp.take_along_axis(position - start_pos, jnp.argsort(sort_order, axis=-1), axis=-1)
    source = jnp.arange(EP_SIZE)[:, None]
    slot_ids = jnp.where(slot_rank < CAP_SLOTS, source * CAP_SLOTS + slot_rank, -1)
    return expert_ids.reshape(SEQS, SEQ_LEN, TOP_K), slot_ids.reshape(SEQS, SEQ_LEN, TOP_K)


def draw_routing(key):
    key_hot, key_score = jax.random.split(key)
    hot_draw = jax.random.randint(key_hot, (STAGES * MICRO_BATCHES, EXPERTS), 0, 1 << 20)
    group_keys = jax.random.split(key_score, STAGES * MICRO_BATCHES)
    expert_ids, slot_ids = lax.map(route_group, (group_keys, hot_draw))
    route_shape = (STAGES, MICRO_BATCHES, SEQS, SEQ_LEN, TOP_K)
    return expert_ids.reshape(route_shape), slot_ids.reshape(route_shape)


def setup_inputs(seed: int = 0, part: int = 0) -> dict:
    base_key = jax.random.key(seed)
    part_keys = jax.random.split(jax.random.fold_in(base_key, part), 5)
    expert_ids, slot_ids = draw_routing(part_keys[0])
    route_shape = (STAGES, MICRO_BATCHES, SEQS, SEQ_LEN, TOP_K)
    gate_draw = jax.random.normal(part_keys[1], route_shape, jnp.float32)
    gate_weights = jnp.exp(1.2 * gate_draw - 0.72) / TOP_K
    expert_scale = jax.random.uniform(part_keys[2], (STAGES * MICRO_BATCHES, EXPERTS, 1, 1), jnp.float32, 0.5, 3.0)
    out_keys = jax.random.split(part_keys[3], STAGES * MICRO_BATCHES)

    def draw_outputs(group_args):
        group_key, group_scale = group_args
        normal_draw = jax.random.normal(group_key, (EXPERTS, SLOTS, D_MODEL), jnp.float32)
        return (normal_draw * group_scale).astype(jnp.bfloat16)

    expert_out = lax.map(draw_outputs, (out_keys, expert_scale)).reshape(STAGES, MICRO_BATCHES, EXPERTS, SLOTS, D_MODEL)
    residual = jax.random.normal(part_keys[4], (STAGES, MICRO_BATCHES, SEQS, SEQ_LEN, D_MODEL), jnp.float32).astype(jnp.bfloat16)
    weight_keys = jax.random.split(jax.random.key(seed + 1), 9)
    in_scale = 1.0 / math.sqrt(D_MODEL)
    down_scale = 2.0 / math.sqrt(FF_SHARED)
    query_scale = 1.5 / math.sqrt(D_MODEL)
    out_scale = math.sqrt(math.sqrt(SEQ_LEN)) / math.sqrt(HEADS_WIDTH)
    norm_moe = jax.random.uniform(weight_keys[0], (STAGES, D_MODEL), jnp.float32, 0.5, 1.5)
    w_gate = (jax.random.normal(weight_keys[1], (STAGES, D_MODEL, FF_SHARED), jnp.float32) * in_scale).astype(jnp.bfloat16)
    w_up = (jax.random.normal(weight_keys[2], (STAGES, D_MODEL, FF_SHARED), jnp.float32) * in_scale).astype(jnp.bfloat16)
    w_down = (jax.random.normal(weight_keys[3], (STAGES, FF_SHARED, D_MODEL), jnp.float32) * down_scale).astype(jnp.bfloat16)
    norm_attn = jax.random.uniform(weight_keys[4], (STAGES, D_MODEL), jnp.float32, 0.5, 1.5)
    w_query = (jax.random.normal(weight_keys[5], (STAGES, D_MODEL, NUM_HEADS, HEAD_DIM), jnp.float32) * query_scale).astype(jnp.bfloat16)
    w_key = (jax.random.normal(weight_keys[6], (STAGES, D_MODEL, NUM_HEADS, HEAD_DIM), jnp.float32) * in_scale).astype(jnp.bfloat16)
    w_value = (jax.random.normal(weight_keys[7], (STAGES, D_MODEL, NUM_HEADS, HEAD_DIM), jnp.float32) * in_scale).astype(jnp.bfloat16)
    w_out = (jax.random.normal(weight_keys[8], (STAGES, NUM_HEADS, HEAD_DIM, D_MODEL), jnp.float32) * out_scale).astype(jnp.bfloat16)
    return {"expert_out": expert_out, "expert_ids": expert_ids, "slot_ids": slot_ids, "gate_weights": gate_weights, "residual": residual, "norm_moe": norm_moe, "w_gate": w_gate, "w_up": w_up, "w_down": w_down, "norm_attn": norm_attn, "w_query": w_query, "w_key": w_key, "w_value": w_value, "w_out": w_out}


def rms_norm(tensor, gain):
    values = tensor.astype(jnp.float32)
    inv_rms = lax.rsqrt(jnp.mean(values * values, axis=-1, keepdims=True) + EPSILON)
    return values * inv_rms * gain


def shared_expert(residual, norm_moe, w_gate, w_up, w_down):
    normed = rms_norm(residual, norm_moe).astype(jnp.bfloat16)
    gate_act = jnp.dot(normed, w_gate, preferred_element_type=jnp.float32)
    up_act = jnp.dot(normed, w_up, preferred_element_type=jnp.float32)
    hidden = (jax.nn.silu(gate_act) * up_act).astype(jnp.bfloat16)
    return jnp.dot(hidden, w_down, preferred_element_type=jnp.float32).astype(jnp.bfloat16)


def combine_micro(micro_args, stage_weights):
    expert_out, expert_ids, slot_ids, gate_weights, residual = micro_args
    norm_moe, w_gate, w_up, w_down = stage_weights
    flat_slots = slot_ids.reshape(TOKENS, TOP_K)
    kept_mask = flat_slots >= 0
    row_ids = expert_ids.reshape(TOKENS, TOP_K) * SLOTS + jnp.where(kept_mask, flat_slots, 0)
    picked = jnp.take(expert_out.reshape(EXPERTS * SLOTS, D_MODEL), row_ids, axis=0)
    weights = jnp.where(kept_mask, gate_weights.reshape(TOKENS, TOP_K), 0.0)
    routed = jnp.sum(picked.astype(jnp.float32) * weights[:, :, None], axis=1)
    flat_resid = residual.reshape(TOKENS, D_MODEL)
    shared = shared_expert(flat_resid, norm_moe, w_gate, w_up, w_down)
    combined = flat_resid.astype(jnp.float32) + shared.astype(jnp.float32) + routed
    return combined.astype(jnp.bfloat16).reshape(SEQS, SEQ_LEN, D_MODEL)


def attend_sequence(seq_args):
    queries, key_heads, value_heads = seq_args
    scores = jnp.einsum("qhe,khe->hqk", queries.astype(jnp.float32), key_heads.astype(jnp.float32)) * SCORE_SCALE
    causal = jnp.arange(SEQ_LEN)[:, None] >= jnp.arange(SEQ_LEN)[None, :]
    scores = jnp.where(causal, scores, -1e30)
    attn_probs = jnp.exp(scores - jnp.max(scores, axis=-1, keepdims=True))
    prob_sum = jnp.sum(attn_probs, axis=-1, keepdims=True)
    attn_mixed = jnp.einsum("hqk,khe->hqe", attn_probs.astype(jnp.bfloat16).astype(jnp.float32), value_heads.astype(jnp.float32))
    return attn_mixed / prob_sum


def attention_stage(stage_args):
    received, norm_attn, w_query, w_key, w_value, w_out = stage_args
    seq_count = MICRO_BATCHES * SEQS
    normed = rms_norm(received, norm_attn).astype(jnp.bfloat16).reshape(seq_count * SEQ_LEN, D_MODEL)

    def project(weight):
        product = jnp.dot(normed, weight.reshape(D_MODEL, HEADS_WIDTH), preferred_element_type=jnp.float32)
        return product.astype(jnp.bfloat16).reshape(seq_count, SEQ_LEN, NUM_HEADS, HEAD_DIM)

    attn_mixed = lax.map(attend_sequence, (project(w_query), project(w_key), project(w_value)))
    mixed_rows = jnp.transpose(attn_mixed.astype(jnp.bfloat16), (0, 2, 1, 3)).reshape(seq_count * SEQ_LEN, HEADS_WIDTH)
    attn_proj = jnp.dot(mixed_rows, w_out.reshape(HEADS_WIDTH, D_MODEL), preferred_element_type=jnp.float32).astype(jnp.bfloat16)
    updated = received.astype(jnp.float32) + attn_proj.astype(jnp.float32).reshape(received.shape)
    return updated.astype(jnp.bfloat16)


def reference(expert_out, expert_ids, slot_ids, gate_weights, residual, norm_moe, w_gate, w_up, w_down, norm_attn, w_query, w_key, w_value, w_out):
    def combine_stage(stage_args):
        def one_micro(micro_args):
            return combine_micro(micro_args, stage_args[5:])
        return lax.map(one_micro, stage_args[:5])

    combined = lax.map(combine_stage, (expert_out, expert_ids, slot_ids, gate_weights, residual, norm_moe, w_gate, w_up, w_down))
    received = jnp.roll(combined, 1, axis=0)
    return lax.map(attention_stage, (received, norm_attn, w_query, w_key, w_value, w_out))
```

```python
import math
import jax
import jax.numpy as jnp
from jax import lax
from jax.experimental import pallas as pl
from jax.experimental.pallas import tpu as pltpu
from jax.sharding import PartitionSpec as P

EPSILON = 1e-6
LANES = 128
CHUNKS = (2, 2, 2, 3)
ROWS = 64
VMEM_LIMIT = 60 << 20
ANY = pl.BlockSpec(memory_space=pl.ANY)


def normalize(blocks, gain, deps=()):
    dim = blocks[0].shape[1]
    step = blocks[0].shape[0]
    counts = [block.shape[0] // step for block in blocks]
    starts = [sum(counts[:c]) for c in range(len(blocks))]
    total = sum(counts)

    def body(*refs):
        sources, gain_ref, out_ref = refs[:len(blocks)], refs[len(blocks)], refs[-1]
        s = pl.program_id(0)
        for ref, start, count in zip(sources, starts, counts):
            @pl.when((s >= start) & (s < start + count))
            def _():
                values = ref[...].astype(jnp.float32)
                inv_rms = lax.rsqrt(jnp.mean(values * values, axis=-1, keepdims=True) + EPSILON)
                out_ref[...] = (values * inv_rms * gain_ref[...]).astype(jnp.bfloat16)

    def spec(start, count):
        return pl.BlockSpec((step, dim), lambda s: (jnp.clip(s - start, 0, count - 1), 0))

    return pl.pallas_call(
        body,
        out_shape=jax.ShapeDtypeStruct((total * step, dim), jnp.bfloat16),
        grid=(total,),
        in_specs=[spec(*pair) for pair in zip(starts, counts)] + [pl.BlockSpec((1, dim), lambda s: (0, 0))] + [ANY] * len(deps),
        out_specs=pl.BlockSpec((step, dim), lambda s: (s, 0)),
        cost_estimate=pl.CostEstimate(flops=1_000_000_000, bytes_accessed=4 * total * step * dim, transcendentals=0),
        name="normalize",
    )(*blocks, gain, *deps)


def gated_hidden(residual, part, parts, gain, w_gate, w_up, deps=()):
    rows, dim = residual.shape[0] // parts, residual.shape[1]
    width = w_gate.shape[1]
    block = 384
    cols = 256

    def gated(res_ref, gain_ref, gate_ref, up_ref, *rest):
        hidden_ref, normed = rest[-2:]

        @pl.when(pl.program_id(0) == 0)
        def _():
            def scale_rows(r, carry):
                at = pl.ds(pl.multiple_of(r * ROWS, ROWS), ROWS)
                values = res_ref[at, :].astype(jnp.float32)
                inv_rms = lax.rsqrt(jnp.mean(values * values, axis=-1, keepdims=True) + EPSILON)
                normed[at, :] = (values * inv_rms * gain_ref[...]).astype(jnp.bfloat16)
                return carry

            lax.fori_loop(0, rows // ROWS, scale_rows, 0)

        def product(r, carry):
            at = pl.ds(pl.multiple_of(r * block, block), block)
            gate_act = jnp.dot(normed[at, :], gate_ref[...], preferred_element_type=jnp.float32)
            up_act = jnp.dot(normed[at, :], up_ref[...], preferred_element_type=jnp.float32)
            hidden_ref[at, :] = (jax.nn.silu(gate_act) * up_act).astype(jnp.bfloat16)
            return carry

        lax.fori_loop(0, rows // block, product, 0)

    return pl.pallas_call(
        gated,
        out_shape=jax.ShapeDtypeStruct((rows, width), jnp.bfloat16),
        grid=(width // cols,),
        in_specs=[
            pl.BlockSpec((rows, dim), lambda n: (part, 0), pipeline_mode=pl.Buffered(1)),
            pl.BlockSpec((1, dim), lambda n: (0, 0)),
            pl.BlockSpec((dim, cols), lambda n: (0, n)),
            pl.BlockSpec((dim, cols), lambda n: (0, n)),
        ] + [ANY] * len(deps),
        out_specs=pl.BlockSpec((rows, cols), lambda n: (0, n)),
        scratch_shapes=[pltpu.VMEM((rows, dim), jnp.bfloat16)],
        compiler_params=pltpu.CompilerParams(vmem_limit_bytes=VMEM_LIMIT),
        cost_estimate=pl.CostEstimate(flops=4 * rows * dim * width, bytes_accessed=4 * dim * width, transcendentals=0),
        name="gated",
    )(residual, gain, w_gate, w_up, *deps)


def down_product(hidden, w_down, deps=()):
    rows, width = hidden.shape
    dim = w_down.shape[1]
    block = 384
    out_cols = 512

    def down(hidden_ref, w_ref, *rest):
        out_ref = rest[-1]

        def product(r, carry):
            at = pl.ds(pl.multiple_of(r * block, block), block)
            out_ref[at, :] = jnp.dot(hidden_ref[at, :], w_ref[...], preferred_element_type=jnp.float32).astype(jnp.bfloat16)
            return carry

        lax.fori_loop(0, rows // block, product, 0)

    return pl.pallas_call(
        down,
        out_shape=jax.ShapeDtypeStruct((rows, dim), jnp.bfloat16),
        grid=(dim // out_cols,),
        in_specs=[
            pl.BlockSpec((rows, width), lambda n: (0, 0), pipeline_mode=pl.Buffered(1)),
            pl.BlockSpec((width, out_cols), lambda n: (0, n)),
        ] + [ANY] * len(deps),
        out_specs=pl.BlockSpec((rows, out_cols), lambda n: (0, n)),
        compiler_params=pltpu.CompilerParams(vmem_limit_bytes=VMEM_LIMIT),
        cost_estimate=pl.CostEstimate(flops=2 * rows * dim * width, bytes_accessed=2 * dim * width, transcendentals=0),
        name="down",
    )(hidden, w_down, *deps)


def attend(queries, keys, values, row_block, blocks, w_out, micro, micro_count, seq_len, head_dim, previous=None, deps=()):
    width = queries.shape[1]
    dim = w_out.shape[1]
    cols = 1024
    group = 4
    pair = 2 * seq_len
    core_steps = width // (group * head_dim)
    scale = 1.0 / math.sqrt(head_dim)
    sizes = [block.shape[0] for block in blocks]
    starts = [sum(sizes[:c]) for c in range(len(sizes))]
    tokens = sum(sizes)

    def body(q_ref, k_ref, v_ref, w_ref, *rest):
        y_refs = rest[:len(blocks)]
        out_ref, mixed = rest[-2], rest[-1]
        s = pl.program_id(0)

        @pl.when(s < core_steps)
        def _():
            row = lax.broadcasted_iota(jnp.int32, (pair, pair), 0)
            col = lax.broadcasted_iota(jnp.int32, (pair, pair), 1)
            visible = (row >= col) & ((row < seq_len) | (col >= seq_len))
            tiles = [(slice(p * pair, (p + 1) * pair), slice(h * head_dim, (h + 1) * head_dim), h) for h in range(group) for p in range(tokens // pair)]
            scores = [lax.dot_general(q_ref[r, c], k_ref[r, c], (((1,), (1,)), ((), ())), preferred_element_type=jnp.float32) * scale for r, c, _ in tiles]
            scores = [jnp.where(visible, score, -1e30) for score in scores]
            probs = [jnp.exp(score - jnp.max(score, axis=-1, keepdims=True)) for score in scores]
            totals = [jnp.sum(prob, axis=-1, keepdims=True) for prob in probs]
            outs = [jnp.dot(prob.astype(jnp.bfloat16), v_ref[r, c], preferred_element_type=jnp.float32) for prob, (r, c, _) in zip(probs, tiles)]
            for out, total, (r, _, h) in zip(outs, totals, tiles):
                mixed[r, pl.ds(pl.multiple_of((s * group + h) * head_dim, head_dim), head_dim)] = (out / total).astype(jnp.bfloat16)

        @pl.when(s >= core_steps)
        def _():
            proj = jnp.dot(mixed[...], w_ref[...], preferred_element_type=jnp.float32).astype(jnp.bfloat16)
            for ref, start, size in zip(y_refs, starts, sizes):
                part = proj[start:start + size].astype(jnp.float32)
                out_ref[0, start:start + size, :] = (ref[...].astype(jnp.float32) + part).astype(jnp.bfloat16)

    core_spec = pl.BlockSpec((tokens, group * head_dim), lambda s: (row_block, jnp.minimum(s, core_steps - 1)))
    tail = lambda s: jnp.maximum(s - core_steps, 0)
    extra = list(deps) + ([] if previous is None else [previous])
    aliases = {} if previous is None else {4 + len(blocks) + len(deps): 0}
    return pl.pallas_call(
        body,
        out_shape=jax.ShapeDtypeStruct((micro_count, tokens, dim), jnp.bfloat16),
        grid=(core_steps + dim // cols,),
        in_specs=[core_spec, core_spec, core_spec, pl.BlockSpec((width, cols), lambda s: (0, tail(s)))]
        + [pl.BlockSpec((size, cols), lambda s: (0, tail(s))) for size in sizes] + [ANY] * len(extra),
        out_specs=pl.BlockSpec((1, tokens, cols), lambda s: (micro, 0, tail(s))),
        scratch_shapes=[pltpu.VMEM((tokens, width), jnp.bfloat16)],
        input_output_aliases=aliases,
        compiler_params=pltpu.CompilerParams(vmem_limit_bytes=VMEM_LIMIT),
        cost_estimate=pl.CostEstimate(flops=2 * tokens * width * dim, bytes_accessed=2 * width * dim, transcendentals=0),
        name="attend",
    )(queries, keys, values, w_out, *blocks, *extra)


def pick_rows(expert_out, picks, cap, deps=()):
    experts, _, dim = expert_out.shape[2:]
    step = 8
    count = len(picks)

    def body(owners_ref, *refs):
        for source_ref, out_ref in zip(refs[:count], refs[-count:]):
            out_ref[...] = source_ref[0, 0]

    def source(which, micro):
        return pl.BlockSpec((1, 1, step, cap, dim), lambda s, o: (0, micro, s, o[which], 0))

    return pl.pallas_call(
        body,
        out_shape=[jax.ShapeDtypeStruct((experts, cap, dim), expert_out.dtype)] * count,
        grid_spec=pltpu.PrefetchScalarGridSpec(
            num_scalar_prefetch=1,
            grid=(experts // step,),
            in_specs=[source(which, micro) for which, (micro, _) in enumerate(picks)] + [ANY] * len(deps),
            out_specs=[pl.BlockSpec((step, cap, dim), lambda s, o: (s, 0, 0))] * count,
        ),
        cost_estimate=pl.CostEstimate(flops=2_000_000_000 * count, bytes_accessed=4 * experts * cap * dim * count, transcendentals=0),
        name="pick",
    )(jnp.stack([owner for _, owner in picks]).astype(jnp.int32), *([expert_out] * count), *deps)


def chip_partial(expert_out, sibling_rows, micro, owner, rows, gates, tokens, top_k, chunks, deps=()):
    experts, cap, dim = sibling_rows.shape
    step = 16
    tiles = dim // LANES
    half = experts // step
    pitch = 2 * experts * cap + 1
    parts = tokens // chunks // ROWS

    def body(owner_ref, rows_ref, gates_ref, own_ref, sib_ref, *rest):
        outs, table = rest[len(deps):-1], rest[-1]
        s = pl.program_id(0)

        def put(ref, base):
            for e in range(step):
                for j in range(tiles):
                    table[pl.ds(j * pitch + base + e * cap, cap), :] = ref[e, :, j * LANES:(j + 1) * LANES].astype(jnp.float32)

        base = pl.multiple_of(s * (step * cap), 8)

        @pl.when(s < half)
        def _():
            put(own_ref.at[0, 0], base)

        @pl.when((s >= half) & (s < 2 * half))
        def _():
            put(sib_ref, base)

        for c, out_ref in enumerate(outs):
            first = 2 * half + c * parts

            @pl.when((s >= first) & (s < first + parts))
            def _():
                def token(t, carry):
                    acc = None
                    for j in range(top_k):
                        at = ((s - 2 * half) * ROWS + t) * top_k + j
                        term = table[pl.ds(rows_ref[at], tiles, stride=pitch), :] * gates_ref[at]
                        acc = term if acc is None else acc + term
                    out_ref[pl.ds(pl.multiple_of(t * tiles, tiles), tiles), :] = acc
                    return carry

                lax.fori_loop(0, ROWS, token, 0, unroll=4)

    def out_spec(c):
        return pl.BlockSpec((ROWS * tiles, LANES), lambda s, o, r, g: (jnp.clip(s - 2 * half - c * parts, 0, parts - 1), 0))

    return pl.pallas_call(
        body,
        out_shape=[jax.ShapeDtypeStruct((parts * ROWS * tiles, LANES), jnp.float32)] * chunks,
        grid_spec=pltpu.PrefetchScalarGridSpec(
            num_scalar_prefetch=3,
            grid=(2 * half + chunks * parts,),
            in_specs=[
                pl.BlockSpec((1, 1, step, cap, dim), lambda s, o, r, g: (0, micro, jnp.minimum(s, half - 1), o[0], 0)),
                pl.BlockSpec((step, cap, dim), lambda s, o, r, g: (jnp.clip(s - half, 0, half - 1), 0, 0)),
            ] + [ANY] * len(deps),
            out_specs=[out_spec(c) for c in range(chunks)],
            scratch_shapes=[pltpu.VMEM((tiles * pitch, LANES), jnp.float32)],
        ),
        compiler_params=pltpu.CompilerParams(vmem_limit_bytes=VMEM_LIMIT),
        cost_estimate=pl.CostEstimate(flops=8_000_000_000, bytes_accessed=3 * experts * cap * dim * 2, transcendentals=0),
        name="combine",
    )(owner, rows, gates, expert_out, sibling_rows, *deps)


def combine_chunk(own_part, far_part, residual, shared, start, sh_start, deps=()):
    dim = residual.shape[1]
    tiles = dim // LANES
    chunk = own_part.shape[0] // tiles
    pitch = ROWS + 2

    def body(own_ref, far_ref, res_ref, sh_ref, *rest):
        out_ref, planes = rest[-2:]

        def token(t, carry):
            at = pl.ds(pl.multiple_of(t * tiles, tiles), tiles)
            planes[pl.ds(t, tiles, stride=pitch), :] = own_ref[at, :] + far_ref[at, :]
            return carry

        lax.fori_loop(0, ROWS, token, 0, unroll=8)
        for j in range(tiles):
            at = slice(j * LANES, (j + 1) * LANES)
            total = res_ref[:, at].astype(jnp.float32) + sh_ref[:, at].astype(jnp.float32) + planes[j * pitch:j * pitch + ROWS, :]
            out_ref[:, at] = total.astype(jnp.bfloat16)

    part_spec = pl.BlockSpec((ROWS * tiles, LANES), lambda s: (s, 0))
    rows_from = lambda first: pl.BlockSpec((ROWS, dim), lambda s: (first // ROWS + s, 0))
    return pl.pallas_call(
        body,
        out_shape=jax.ShapeDtypeStruct((chunk, dim), jnp.bfloat16),
        grid=(chunk // ROWS,),
        in_specs=[part_spec, part_spec, rows_from(start), rows_from(sh_start)] + [ANY] * len(deps),
        out_specs=pl.BlockSpec((ROWS, dim), lambda s: (s, 0)),
        scratch_shapes=[pltpu.VMEM((tiles * pitch, LANES), jnp.float32)],
        cost_estimate=pl.CostEstimate(flops=1_000_000_000, bytes_accessed=14 * chunk * dim, transcendentals=0),
        name="finish",
    )(own_part, far_part, residual, shared, *deps)


def solution(mesh):
    stages = mesh.shape["pp"]
    ep_size = mesh.shape["ep"]
    shift_pairs = [(source, (source + 1) % stages) for source in range(stages)]
    core_pairs = [(source, source ^ 1) for source in range(ep_size)]
    chip_pairs = [(source, (source + 2) % ep_size) for source in range(ep_size)]
    tok_spec = P("pp", "data", "ep", None, None)
    vec_spec = P("pp", None)
    mat_spec = P("pp", None, None)
    head_spec = P("pp", None, None, None)

    def device_step(expert_out, expert_ids, slot_ids, gate_weights, residual, norm_moe, w_gate, w_up, w_down, norm_attn, w_query, w_key, w_value, w_out):
        micro_count, local_experts, slots_total, dim = expert_out.shape[1:]
        seqs, seq_len, top_k = expert_ids.shape[2:]
        tokens = seqs * seq_len
        cap = slots_total // ep_size
        me = lax.axis_index("ep")
        chip, core = me // 2, me % 2
        far = (me + 2) % ep_size
        as_owner = lambda who: jnp.reshape(who, (1,)).astype(jnp.int32)

        home = expert_ids[0] // local_experts
        slot = slot_ids[0]
        row_here = (expert_ids[0] % local_experts) * cap + (slot - me * cap)

        def routing(on_chip):
            usable = (slot >= 0) & (home // 2 == on_chip)
            row = row_here + jnp.where(home % 2 == core, 0, local_experts * cap)
            flat = (micro_count, tokens * top_k)
            return jnp.where(usable, row, 0).reshape(flat), jnp.where(usable, gate_weights[0], 0.0).reshape(flat)

        own_rows, own_gates = routing(chip)
        send_rows, send_gates = routing(1 - chip)
        far_meta = lax.ppermute(jnp.stack([send_rows.astype(jnp.float32), send_gates]), "ep", chip_pairs)
        far_rows, far_gates = far_meta[0].astype(jnp.int32), far_meta[1]

        to_far = lambda m: (m, far ^ 1)
        to_own = lambda m: (m, me ^ 1)
        pick_plan = ([to_far(0)], [to_far(1)], [to_far(2), to_own(0)], [to_far(3), to_own(1)], [to_own(2), to_own(3)])
        from_sibling = []

        def exchange(step, deps):
            picked = pick_rows(expert_out, pick_plan[step], cap, deps)
            from_sibling.append([lax.ppermute(rows, "ep", core_pairs) for rows in picked])
            return (picked[-1],)

        last = exchange(1, exchange(0, ()))
        arrived = []
        for m in range(micro_count):
            parts = chip_partial(expert_out, from_sibling[m][0], m, as_owner(far), far_rows[m], far_gates[m], tokens, top_k, CHUNKS[m], last)
            last = (parts[0],)
            arrived.append([])
            for part in parts:
                arrived[m].append(lax.ppermute(part, "ep", chip_pairs))
            if m + 2 < len(pick_plan):
                last = exchange(m + 2, last)
        own_sib = [from_sibling[2][1], from_sibling[3][1], *from_sibling[4]]

        flat_resid = residual.reshape(micro_count * tokens, dim)
        heads_width = w_query.shape[2] * w_query.shape[3]
        flat = lambda weight: weight[0].reshape(dim, heads_width)

        def own(m, deps):
            return chip_partial(expert_out, own_sib[m], m, as_owner(me), own_rows[m], own_gates[m], tokens, top_k, CHUNKS[m], deps)

        halves = 2
        half_tokens = micro_count * tokens // halves
        hidden_half = lambda part, deps: gated_hidden(flat_resid, part, halves, norm_moe, w_gate[0], w_up[0], deps)
        shared = [down_product(hidden_half(0, last), w_down[0])]
        here = [None] * micro_count
        pieces = [[] for _ in range(micro_count)]

        def finish(m, c, deps):
            chunk = tokens // CHUNKS[m]
            start = m * tokens + c * chunk
            combined = combine_chunk(here[m][c], arrived[m][c], flat_resid, shared[start // half_tokens], start, start % half_tokens, deps)
            pieces[m].append(lax.ppermute(combined, "pp", shift_pairs))
            return (combined,)

        def project(micros, deps):
            normed = normalize([piece for m in micros for piece in pieces[m]], norm_attn, deps)
            return [jnp.dot(normed, flat(weight), preferred_element_type=jnp.float32).astype(jnp.bfloat16) for weight in (w_query, w_key, w_value)]

        def mix(m, row_block, projected, previous, deps):
            return attend(*projected, row_block, pieces[m], w_out[0].reshape(heads_width, dim), m, micro_count, seq_len, w_query.shape[3], previous, deps)

        here[0] = own(0, (shared[0],))
        last = finish(0, 1, finish(0, 0, (here[0][0],)))
        hidden = hidden_half(1, last)
        here[1] = own(1, (hidden,))
        last = finish(1, 0, (here[1][0],))
        shared.append(down_product(hidden, w_down[0], last))
        last = finish(1, 1, (shared[1],))
        here[2] = own(2, last)
        here[3] = own(3, (here[2][0],))
        both = project((0, 1), (here[3][0],))
        last = finish(2, 1, finish(2, 0, tuple(both)))
        out = mix(0, 0, both, None, last)
        out = mix(1, 1, both, out, ())
        last = finish(3, 1, finish(3, 0, (out,)))
        third = project((2,), last)
        last = finish(3, 2, tuple(third))
        out = mix(2, 0, third, out, last)
        fourth = project((3,), (out,))
        out = mix(3, 0, fourth, out, ())
        return out.reshape(residual.shape)

    in_specs = (tok_spec,) * 5 + (vec_spec, mat_spec, mat_spec, mat_spec, vec_spec, head_spec, head_spec, head_spec, head_spec)

    return jax.shard_map(device_step, mesh=mesh, in_specs=in_specs, out_specs=tok_spec, check_vma=False)
```

```python
import math
import jax
import jax.numpy as jnp
from jax import lax
from jax.experimental import pallas as pl
from jax.experimental.pallas import tpu as pltpu
from jax.sharding import PartitionSpec as P

EPSILON = 1e-6
LANES = 128
CHUNKS = (1, 3, 2, 3)
ROWS = 64
VMEM_LIMIT = 60 << 20
ANY = pl.BlockSpec(memory_space=pl.ANY)


def normalize(blocks, gain, deps=()):
    dim = blocks[0].shape[1]
    step = math.gcd(*[block.shape[0] for block in blocks])
    counts = [block.shape[0] // step for block in blocks]
    starts = [sum(counts[:c]) for c in range(len(blocks))]
    total = sum(counts)

    def body(*refs):
        sources, gain_ref, out_ref = refs[:len(blocks)], refs[len(blocks)], refs[-1]
        s = pl.program_id(0)
        for ref, start, count in zip(sources, starts, counts):
            @pl.when((s >= start) & (s < start + count))
            def _():
                values = ref[...].astype(jnp.float32)
                inv_rms = lax.rsqrt(jnp.mean(values * values, axis=-1, keepdims=True) + EPSILON)
                out_ref[...] = (values * inv_rms * gain_ref[...]).astype(jnp.bfloat16)

    def spec(start, count):
        return pl.BlockSpec((step, dim), lambda s: (jnp.clip(s - start, 0, count - 1), 0))

    return pl.pallas_call(
        body,
        out_shape=jax.ShapeDtypeStruct((total * step, dim), jnp.bfloat16),
        grid=(total,),
        in_specs=[spec(*pair) for pair in zip(starts, counts)] + [pl.BlockSpec((1, dim), lambda s: (0, 0))] + [ANY] * len(deps),
        out_specs=pl.BlockSpec((step, dim), lambda s: (s, 0)),
        cost_estimate=pl.CostEstimate(flops=1_000_000_000, bytes_accessed=4 * total * step * dim, transcendentals=0),
        name="normalize",
    )(*blocks, gain, *deps)


def gated_hidden(residual, part, parts, gain, w_gate, w_up, deps=()):
    rows, dim = residual.shape[0] // parts, residual.shape[1]
    width = w_gate.shape[1]
    block = 768
    cols = 256

    def gated(res_ref, gain_ref, gate_ref, up_ref, *rest):
        hidden_ref, normed = rest[-2:]

        @pl.when(pl.program_id(0) == 0)
        def _():
            def scale_rows(r, carry):
                at = pl.ds(pl.multiple_of(r * ROWS, ROWS), ROWS)
                values = res_ref[at, :].astype(jnp.float32)
                inv_rms = lax.rsqrt(jnp.mean(values * values, axis=-1, keepdims=True) + EPSILON)
                normed[at, :] = (values * inv_rms * gain_ref[...]).astype(jnp.bfloat16)
                return carry

            lax.fori_loop(0, rows // ROWS, scale_rows, 0)

        def product(r, carry):
            at = pl.ds(pl.multiple_of(r * block, block), block)
            gate_act = jnp.dot(normed[at, :], gate_ref[...], preferred_element_type=jnp.float32)
            up_act = jnp.dot(normed[at, :], up_ref[...], preferred_element_type=jnp.float32)
            hidden_ref[at, :] = (jax.nn.silu(gate_act) * up_act).astype(jnp.bfloat16)
            return carry

        lax.fori_loop(0, rows // block, product, 0)

    return pl.pallas_call(
        gated,
        out_shape=jax.ShapeDtypeStruct((rows, width), jnp.bfloat16),
        grid=(width // cols,),
        in_specs=[
            pl.BlockSpec((rows, dim), lambda n: (part, 0), pipeline_mode=pl.Buffered(1)),
            pl.BlockSpec((1, dim), lambda n: (0, 0)),
            pl.BlockSpec((dim, cols), lambda n: (0, n)),
            pl.BlockSpec((dim, cols), lambda n: (0, n)),
        ] + [ANY] * len(deps),
        out_specs=pl.BlockSpec((rows, cols), lambda n: (0, n)),
        scratch_shapes=[pltpu.VMEM((rows, dim), jnp.bfloat16)],
        compiler_params=pltpu.CompilerParams(vmem_limit_bytes=VMEM_LIMIT),
        cost_estimate=pl.CostEstimate(flops=4 * rows * dim * width, bytes_accessed=4 * dim * width, transcendentals=0),
        name="gated",
    )(residual, gain, w_gate, w_up, *deps)


def down_product(hidden, w_down, deps=()):
    rows, width = hidden.shape
    dim = w_down.shape[1]
    block = 768
    out_cols = 512

    def down(hidden_ref, w_ref, *rest):
        out_ref = rest[-1]

        def product(r, carry):
            at = pl.ds(pl.multiple_of(r * block, block), block)
            out_ref[at, :] = jnp.dot(hidden_ref[at, :], w_ref[...], preferred_element_type=jnp.float32).astype(jnp.bfloat16)
            return carry

        lax.fori_loop(0, rows // block, product, 0)

    return pl.pallas_call(
        down,
        out_shape=jax.ShapeDtypeStruct((rows, dim), jnp.bfloat16),
        grid=(dim // out_cols,),
        in_specs=[
            pl.BlockSpec((rows, width), lambda n: (0, 0), pipeline_mode=pl.Buffered(1)),
            pl.BlockSpec((width, out_cols), lambda n: (0, n)),
        ] + [ANY] * len(deps),
        out_specs=pl.BlockSpec((rows, out_cols), lambda n: (0, n)),
        compiler_params=pltpu.CompilerParams(vmem_limit_bytes=VMEM_LIMIT),
        cost_estimate=pl.CostEstimate(flops=2 * rows * dim * width, bytes_accessed=2 * dim * width, transcendentals=0),
        name="down",
    )(hidden, w_down, *deps)


def attend(queries, keys, values, row_block, blocks, w_out, micro, micro_count, seq_len, head_dim, previous=None, deps=()):
    width = queries.shape[1]
    dim = w_out.shape[1]
    cols = 1024
    group = 8
    pair = 2 * seq_len
    core_steps = width // (group * head_dim)
    scale = 1.0 / math.sqrt(head_dim)
    sizes = [block.shape[0] for block in blocks]
    starts = [sum(sizes[:c]) for c in range(len(sizes))]
    tokens = sum(sizes)

    def body(q_ref, k_ref, v_ref, w_ref, *rest):
        y_refs = rest[:len(blocks)]
        out_ref, mixed = rest[-2], rest[-1]
        s = pl.program_id(0)

        @pl.when(s < core_steps)
        def _():
            row = lax.broadcasted_iota(jnp.int32, (pair, pair), 0)
            col = lax.broadcasted_iota(jnp.int32, (pair, pair), 1)
            visible = (row >= col) & ((row < seq_len) | (col >= seq_len))
            tiles = [(slice(p * pair, (p + 1) * pair), slice(h * head_dim, (h + 1) * head_dim), h) for h in range(group) for p in range(tokens // pair)]
            scores = [lax.dot_general(q_ref[r, c], k_ref[r, c], (((1,), (1,)), ((), ())), preferred_element_type=jnp.float32) * scale for r, c, _ in tiles]
            scores = [jnp.where(visible, score, -1e30) for score in scores]
            probs = [jnp.exp(score - jnp.max(score, axis=-1, keepdims=True)) for score in scores]
            totals = [jnp.sum(prob, axis=-1, keepdims=True) for prob in probs]
            outs = [jnp.dot(prob.astype(jnp.bfloat16), v_ref[r, c], preferred_element_type=jnp.float32) for prob, (r, c, _) in zip(probs, tiles)]
            for out, total, (r, _, h) in zip(outs, totals, tiles):
                mixed[r, pl.ds(pl.multiple_of((s * group + h) * head_dim, head_dim), head_dim)] = (out / total).astype(jnp.bfloat16)

        @pl.when(s >= core_steps)
        def _():
            proj = jnp.dot(mixed[...], w_ref[...], preferred_element_type=jnp.float32).astype(jnp.bfloat16)
            for ref, start, size in zip(y_refs, starts, sizes):
                part = proj[start:start + size].astype(jnp.float32)
                out_ref[0, start:start + size, :] = (ref[...].astype(jnp.float32) + part).astype(jnp.bfloat16)

    core_spec = pl.BlockSpec((tokens, group * head_dim), lambda s: (row_block, jnp.minimum(s, core_steps - 1)))
    tail = lambda s: jnp.maximum(s - core_steps, 0)
    extra = list(deps) + ([] if previous is None else [previous])
    aliases = {} if previous is None else {4 + len(blocks) + len(deps): 0}
    return pl.pallas_call(
        body,
        out_shape=jax.ShapeDtypeStruct((micro_count, tokens, dim), jnp.bfloat16),
        grid=(core_steps + dim // cols,),
        in_specs=[core_spec, core_spec, core_spec, pl.BlockSpec((width, cols), lambda s: (0, tail(s)))]
        + [pl.BlockSpec((size, cols), lambda s: (0, tail(s))) for size in sizes] + [ANY] * len(extra),
        out_specs=pl.BlockSpec((1, tokens, cols), lambda s: (micro, 0, tail(s))),
        scratch_shapes=[pltpu.VMEM((tokens, width), jnp.bfloat16)],
        input_output_aliases=aliases,
        compiler_params=pltpu.CompilerParams(vmem_limit_bytes=VMEM_LIMIT),
        cost_estimate=pl.CostEstimate(flops=2 * tokens * width * dim, bytes_accessed=2 * width * dim, transcendentals=0),
        name="attend",
    )(queries, keys, values, w_out, *blocks, *extra)


def pick_rows(expert_out, picks, cap, deps=()):
    experts, _, dim = expert_out.shape[2:]
    step = 16
    count = len(picks)

    def body(owners_ref, *refs):
        for source_ref, out_ref in zip(refs[:count], refs[-count:]):
            out_ref[...] = source_ref[0, 0]

    def source(which, micro):
        return pl.BlockSpec((1, 1, step, cap, dim), lambda s, o: (0, micro, s, o[which], 0))

    return pl.pallas_call(
        body,
        out_shape=[jax.ShapeDtypeStruct((experts, cap, dim), expert_out.dtype)] * count,
        grid_spec=pltpu.PrefetchScalarGridSpec(
            num_scalar_prefetch=1,
            grid=(experts // step,),
            in_specs=[source(which, micro) for which, (micro, _) in enumerate(picks)] + [ANY] * len(deps),
            out_specs=[pl.BlockSpec((step, cap, dim), lambda s, o: (s, 0, 0))] * count,
        ),
        cost_estimate=pl.CostEstimate(flops=2_000_000_000 * count, bytes_accessed=4 * experts * cap * dim * count, transcendentals=0),
        name="pick",
    )(jnp.stack([owner for _, owner in picks]).astype(jnp.int32), *([expert_out] * count), *deps)


def chip_partial(expert_out, sibling_rows, micro, owner, rows, gates, tokens, top_k, chunks, deps=()):
    experts, cap, dim = sibling_rows.shape
    step = 4
    streams = 2
    tiles = dim // LANES
    steps = experts // (step * streams)
    pitch = 2 * experts * cap + 1
    count = min(128, tokens // chunks)
    while (tokens // chunks) % count:
        count -= 32
    parts = tokens // chunks // count

    def body(owner_ref, rows_ref, gates_ref, *rest):
        sources = rest[:2 * streams]
        outs, table = rest[2 * streams + len(deps):-1], rest[-1]
        s = pl.program_id(0)

        @pl.when(s < steps)
        def _():
            for k, ref in enumerate(sources):
                base = pl.multiple_of((k * steps + s) * (step * cap), 8)
                for e in range(step):
                    for j in range(tiles):
                        rows_e = ref[0, 0, e, :, j * LANES:(j + 1) * LANES] if k < streams else ref[e, :, j * LANES:(j + 1) * LANES]
                        table[pl.ds(j * pitch + base + e * cap, cap), :] = rows_e.astype(jnp.float32)

        for c, out_ref in enumerate(outs):
            first = steps + c * parts

            @pl.when((s >= first) & (s < first + parts))
            def _():
                def token(t, carry):
                    acc = None
                    for j in range(top_k):
                        at = ((s - steps) * count + t) * top_k + j
                        term = table[pl.ds(rows_ref[at], tiles, stride=pitch), :] * gates_ref[at]
                        acc = term if acc is None else acc + term
                    out_ref[pl.ds(pl.multiple_of(t * tiles, tiles), tiles), :] = acc
                    return carry

                lax.fori_loop(0, count, token, 0, unroll=8)

    def own_spec(k):
        return pl.BlockSpec((1, 1, step, cap, dim), lambda s, o, r, g: (0, micro, k * steps + jnp.minimum(s, steps - 1), o[0], 0))

    def sibling_spec(k):
        return pl.BlockSpec((step, cap, dim), lambda s, o, r, g: (k * steps + jnp.minimum(s, steps - 1), 0, 0))

    def out_spec(c):
        return pl.BlockSpec((count * tiles, LANES), lambda s, o, r, g: (jnp.clip(s - steps - c * parts, 0, parts - 1), 0))

    return pl.pallas_call(
        body,
        out_shape=[jax.ShapeDtypeStruct((parts * count * tiles, LANES), jnp.float32)] * chunks,
        grid_spec=pltpu.PrefetchScalarGridSpec(
            num_scalar_prefetch=3,
            grid=(steps + chunks * parts,),
            in_specs=[own_spec(k) for k in range(streams)] + [sibling_spec(k) for k in range(streams)] + [ANY] * len(deps),
            out_specs=[out_spec(c) for c in range(chunks)],
            scratch_shapes=[pltpu.VMEM((tiles * pitch, LANES), jnp.float32)],
        ),
        compiler_params=pltpu.CompilerParams(vmem_limit_bytes=VMEM_LIMIT),
        cost_estimate=pl.CostEstimate(flops=8_000_000_000, bytes_accessed=3 * experts * cap * dim * 2, transcendentals=0),
        name="combine",
    )(owner, rows, gates, *([expert_out] * streams), *([sibling_rows] * streams), *deps)


def combine_chunk(own_part, far_part, residual, shared, start, sh_start, deps=()):
    dim = residual.shape[1]
    tiles = dim // LANES
    chunk = own_part.shape[0] // tiles
    block = 96 if chunk % 96 == 0 else ROWS
    pitch = block + 2

    def body(own_ref, far_ref, res_ref, sh_ref, *rest):
        out_ref, planes = rest[-2:]

        def token(t, carry):
            at = pl.ds(pl.multiple_of(t * tiles, tiles), tiles)
            planes[pl.ds(t, tiles, stride=pitch), :] = own_ref[at, :] + far_ref[at, :]
            return carry

        lax.fori_loop(0, block, token, 0, unroll=8)
        for j in range(tiles):
            at = slice(j * LANES, (j + 1) * LANES)
            total = res_ref[:, at].astype(jnp.float32) + sh_ref[:, at].astype(jnp.float32) + planes[j * pitch:j * pitch + block, :]
            out_ref[:, at] = total.astype(jnp.bfloat16)

    part_spec = pl.BlockSpec((block * tiles, LANES), lambda s: (s, 0))
    rows_from = lambda first: pl.BlockSpec((block, dim), lambda s: (first // block + s, 0))
    return pl.pallas_call(
        body,
        out_shape=jax.ShapeDtypeStruct((chunk, dim), jnp.bfloat16),
        grid=(chunk // block,),
        in_specs=[part_spec, part_spec, rows_from(start), rows_from(sh_start)] + [ANY] * len(deps),
        out_specs=pl.BlockSpec((block, dim), lambda s: (s, 0)),
        scratch_shapes=[pltpu.VMEM((tiles * pitch, LANES), jnp.float32)],
        cost_estimate=pl.CostEstimate(flops=1_000_000_000, bytes_accessed=14 * chunk * dim, transcendentals=0),
        name="finish",
    )(own_part, far_part, residual, shared, *deps)


def solution(mesh):
    stages = mesh.shape["pp"]
    ep_size = mesh.shape["ep"]
    shift_pairs = [(source, (source + 1) % stages) for source in range(stages)]
    core_pairs = [(source, source ^ 1) for source in range(ep_size)]
    chip_pairs = [(source, (source + 2) % ep_size) for source in range(ep_size)]
    tok_spec = P("pp", "data", "ep", None, None)
    vec_spec = P("pp", None)
    mat_spec = P("pp", None, None)
    head_spec = P("pp", None, None, None)

    def device_step(expert_out, expert_ids, slot_ids, gate_weights, residual, norm_moe, w_gate, w_up, w_down, norm_attn, w_query, w_key, w_value, w_out):
        micro_count, local_experts, slots_total, dim = expert_out.shape[1:]
        seqs, seq_len, top_k = expert_ids.shape[2:]
        tokens = seqs * seq_len
        cap = slots_total // ep_size
        me = lax.axis_index("ep")
        chip, core = me // 2, me % 2
        far = (me + 2) % ep_size
        as_owner = lambda who: jnp.reshape(who, (1,)).astype(jnp.int32)

        home = expert_ids[0] // local_experts
        slot = slot_ids[0]
        row_here = (expert_ids[0] % local_experts) * cap + (slot - me * cap)

        def routing(on_chip):
            usable = (slot >= 0) & (home // 2 == on_chip)
            row = row_here + jnp.where(home % 2 == core, 0, local_experts * cap)
            flat = (micro_count, tokens * top_k)
            return jnp.where(usable, row, 0).reshape(flat), jnp.where(usable, gate_weights[0], 0.0).reshape(flat)

        own_rows, own_gates = routing(chip)
        send_rows, send_gates = routing(1 - chip)
        far_meta = lax.ppermute(jnp.stack([send_rows.astype(jnp.float32), send_gates]), "ep", chip_pairs)
        far_rows, far_gates = far_meta[0].astype(jnp.int32), far_meta[1]

        to_far = lambda m: (m, far ^ 1)
        to_own = lambda m: (m, me ^ 1)
        pick_plan = ([to_far(0)], [to_far(1)], [to_far(2), to_own(0)], [to_far(3), to_own(1)], [to_own(2), to_own(3)])
        from_sibling = []

        def exchange(step, deps):
            picked = pick_rows(expert_out, pick_plan[step], cap, deps)
            from_sibling.append([lax.ppermute(rows, "ep", core_pairs) for rows in picked])
            return (picked[-1],)

        last = exchange(1, exchange(0, ()))
        arrived = []
        for m in range(micro_count):
            parts = chip_partial(expert_out, from_sibling[m][0], m, as_owner(far), far_rows[m], far_gates[m], tokens, top_k, CHUNKS[m], last)
            last = (parts[0],)
            arrived.append([])
            for part in parts:
                arrived[m].append(lax.ppermute(part, "ep", chip_pairs))
            if m + 2 < len(pick_plan):
                last = exchange(m + 2, last)
        own_sib = [from_sibling[2][1], from_sibling[3][1], *from_sibling[4]]

        flat_resid = residual.reshape(micro_count * tokens, dim)
        heads_width = w_query.shape[2] * w_query.shape[3]
        flat = lambda weight: weight[0].reshape(dim, heads_width)

        def own(m, deps):
            return chip_partial(expert_out, own_sib[m], m, as_owner(me), own_rows[m], own_gates[m], tokens, top_k, CHUNKS[m], deps)

        halves = 2
        half_tokens = micro_count * tokens // halves
        hidden_half = lambda part, deps: gated_hidden(flat_resid, part, halves, norm_moe, w_gate[0], w_up[0], deps)
        shared = [down_product(hidden_half(0, last), w_down[0])]
        here = [None] * micro_count
        pieces = [[] for _ in range(micro_count)]

        def finish(m, c, deps):
            chunk = tokens // CHUNKS[m]
            start = m * tokens + c * chunk
            combined = combine_chunk(here[m][c], arrived[m][c], flat_resid, shared[start // half_tokens], start, start % half_tokens, deps)
            pieces[m].append(lax.ppermute(combined, "pp", shift_pairs))
            return (combined,)

        def project(micros, deps):
            normed = normalize([piece for m in micros for piece in pieces[m]], norm_attn, deps)
            return [jnp.dot(normed, flat(weight), preferred_element_type=jnp.float32).astype(jnp.bfloat16) for weight in (w_query, w_key, w_value)]

        def mix(m, row_block, projected, previous, deps):
            return attend(*projected, row_block, pieces[m], w_out[0].reshape(heads_width, dim), m, micro_count, seq_len, w_query.shape[3], previous, deps)

        here[0] = own(0, (shared[0],))
        last = finish(0, 0, (here[0][0],))
        hidden = hidden_half(1, last)
        here[1] = own(1, (hidden,))
        last = finish(1, 1, finish(1, 0, (here[1][0],)))
        shared.append(down_product(hidden, w_down[0], last))
        here[2] = own(2, (shared[1],))
        last = finish(1, 2, (here[2][0],))
        here[3] = own(3, last)
        both = project((0, 1), (here[3][0],))
        last = finish(2, 0, (both[2],))
        last = finish(2, 1, (*both, *last))
        out = mix(0, 0, both, None, last)
        out = mix(1, 1, both, out, ())
        last = finish(3, 0, (out,))
        third = project((2,), last)
        last = finish(3, 1, (third[2],))
        last = finish(3, 2, (third[1], *last))
        out = mix(2, 0, third, out, last)
        fourth = project((3,), (out,))
        out = mix(3, 0, fourth, out, ())
        return out.reshape(residual.shape)

    in_specs = (tok_spec,) * 5 + (vec_spec, mat_spec, mat_spec, mat_spec, vec_spec, head_spec, head_spec, head_spec, head_spec)

    return jax.shard_map(device_step, mesh=mesh, in_specs=in_specs, out_specs=tok_spec, check_vma=False)
```

```python
import math
import jax
import jax.numpy as jnp
from jax import lax
from jax.experimental import pallas as pl
from jax.experimental.pallas import tpu as pltpu
from jax.sharding import PartitionSpec as P

EPSILON = 1e-6
LANES = 128
CHUNKS = (1, 3, 2, 3)
ROWS = 64
VMEM_LIMIT = 60 << 20
ANY = pl.BlockSpec(memory_space=pl.ANY)


def normalize(blocks, gain, deps=()):
    dim = blocks[0].shape[1]
    step = math.gcd(*[block.shape[0] for block in blocks])
    counts = [block.shape[0] // step for block in blocks]
    starts = [sum(counts[:c]) for c in range(len(blocks))]
    total = sum(counts)

    def body(*refs):
        sources, gain_ref, out_ref = refs[:len(blocks)], refs[len(blocks)], refs[-1]
        s = pl.program_id(0)
        for ref, start, count in zip(sources, starts, counts):
            @pl.when((s >= start) & (s < start + count))
            def _():
                values = ref[...].astype(jnp.float32)
                inv_rms = lax.rsqrt(jnp.mean(values * values, axis=-1, keepdims=True) + EPSILON)
                out_ref[...] = (values * inv_rms * gain_ref[...]).astype(jnp.bfloat16)

    def spec(start, count):
        return pl.BlockSpec((step, dim), lambda s: (jnp.clip(s - start, 0, count - 1), 0))

    return pl.pallas_call(
        body,
        out_shape=jax.ShapeDtypeStruct((total * step, dim), jnp.bfloat16),
        grid=(total,),
        in_specs=[spec(*pair) for pair in zip(starts, counts)] + [pl.BlockSpec((1, dim), lambda s: (0, 0))] + [ANY] * len(deps),
        out_specs=pl.BlockSpec((step, dim), lambda s: (s, 0)),
        cost_estimate=pl.CostEstimate(flops=1_000_000_000, bytes_accessed=4 * total * step * dim, transcendentals=0),
        name="normalize",
    )(*blocks, gain, *deps)


def gated_hidden(residual, part, parts, gain, w_gate, w_up, deps=()):
    rows, dim = residual.shape[0] // parts, residual.shape[1]
    width = w_gate.shape[1]
    block = 768
    cols = 256

    def gated(res_ref, gain_ref, gate_ref, up_ref, *rest):
        hidden_ref, normed = rest[-2:]

        @pl.when(pl.program_id(0) == 0)
        def _():
            def scale_rows(r, carry):
                at = pl.ds(pl.multiple_of(r * ROWS, ROWS), ROWS)
                values = res_ref[at, :].astype(jnp.float32)
                inv_rms = lax.rsqrt(jnp.mean(values * values, axis=-1, keepdims=True) + EPSILON)
                normed[at, :] = (values * inv_rms * gain_ref[...]).astype(jnp.bfloat16)
                return carry

            lax.fori_loop(0, rows // ROWS, scale_rows, 0)

        def product(r, carry):
            at = pl.ds(pl.multiple_of(r * block, block), block)
            gate_act = jnp.dot(normed[at, :], gate_ref[...], preferred_element_type=jnp.float32)
            up_act = jnp.dot(normed[at, :], up_ref[...], preferred_element_type=jnp.float32)
            hidden_ref[at, :] = (jax.nn.silu(gate_act) * up_act).astype(jnp.bfloat16)
            return carry

        lax.fori_loop(0, rows // block, product, 0)

    return pl.pallas_call(
        gated,
        out_shape=jax.ShapeDtypeStruct((rows, width), jnp.bfloat16),
        grid=(width // cols,),
        in_specs=[
            pl.BlockSpec((rows, dim), lambda n: (part, 0), pipeline_mode=pl.Buffered(1)),
            pl.BlockSpec((1, dim), lambda n: (0, 0)),
            pl.BlockSpec((dim, cols), lambda n: (0, n)),
            pl.BlockSpec((dim, cols), lambda n: (0, n)),
        ] + [ANY] * len(deps),
        out_specs=pl.BlockSpec((rows, cols), lambda n: (0, n)),
        scratch_shapes=[pltpu.VMEM((rows, dim), jnp.bfloat16)],
        compiler_params=pltpu.CompilerParams(vmem_limit_bytes=VMEM_LIMIT),
        cost_estimate=pl.CostEstimate(flops=4 * rows * dim * width, bytes_accessed=4 * dim * width, transcendentals=0),
        name="gated",
    )(residual, gain, w_gate, w_up, *deps)


def down_product(hidden, w_down, deps=()):
    rows, width = hidden.shape
    dim = w_down.shape[1]
    block = 768
    out_cols = 512

    def down(hidden_ref, w_ref, *rest):
        out_ref = rest[-1]

        def product(r, carry):
            at = pl.ds(pl.multiple_of(r * block, block), block)
            out_ref[at, :] = jnp.dot(hidden_ref[at, :], w_ref[...], preferred_element_type=jnp.float32).astype(jnp.bfloat16)
            return carry

        lax.fori_loop(0, rows // block, product, 0)

    return pl.pallas_call(
        down,
        out_shape=jax.ShapeDtypeStruct((rows, dim), jnp.bfloat16),
        grid=(dim // out_cols,),
        in_specs=[
            pl.BlockSpec((rows, width), lambda n: (0, 0), pipeline_mode=pl.Buffered(1)),
            pl.BlockSpec((width, out_cols), lambda n: (0, n)),
        ] + [ANY] * len(deps),
        out_specs=pl.BlockSpec((rows, out_cols), lambda n: (0, n)),
        compiler_params=pltpu.CompilerParams(vmem_limit_bytes=VMEM_LIMIT),
        cost_estimate=pl.CostEstimate(flops=2 * rows * dim * width, bytes_accessed=2 * dim * width, transcendentals=0),
        name="down",
    )(hidden, w_down, *deps)


def attend(queries, keys, values, blocks, w_out, micro, each, micro_count, seq_len, head_dim, previous=None, deps=()):
    width = queries.shape[1]
    dim = w_out.shape[1]
    cols = 1024
    group = 8 * each // queries.shape[0]
    pair = 2 * seq_len
    core_steps = width // (group * head_dim)
    scale = 1.0 / math.sqrt(head_dim)
    sizes = [block.shape[0] for block in blocks]
    starts = [sum(sizes[:c]) for c in range(len(sizes))]
    tokens = sum(sizes)
    micros = tokens // each

    def body(q_ref, k_ref, v_ref, w_ref, *rest):
        y_refs = rest[:len(blocks)]
        out_ref, mixed = rest[-2], rest[-1]
        s = pl.program_id(0)

        @pl.when(s < core_steps)
        def _():
            row = lax.broadcasted_iota(jnp.int32, (pair, pair), 0)
            col = lax.broadcasted_iota(jnp.int32, (pair, pair), 1)
            visible = (row >= col) & ((row < seq_len) | (col >= seq_len))
            tiles = [(slice(p * pair, (p + 1) * pair), slice(h * head_dim, (h + 1) * head_dim), h) for h in range(group) for p in range(tokens // pair)]
            scores = [lax.dot_general(q_ref[r, c], k_ref[r, c], (((1,), (1,)), ((), ())), preferred_element_type=jnp.float32) * scale for r, c, _ in tiles]
            scores = [jnp.where(visible, score, -1e30) for score in scores]
            probs = [jnp.exp(score - jnp.max(score, axis=-1, keepdims=True)) for score in scores]
            totals = [jnp.sum(prob, axis=-1, keepdims=True) for prob in probs]
            outs = [jnp.dot(prob.astype(jnp.bfloat16), v_ref[r, c], preferred_element_type=jnp.float32) for prob, (r, c, _) in zip(probs, tiles)]
            for out, total, (r, _, h) in zip(outs, totals, tiles):
                mixed[r, pl.ds(pl.multiple_of((s * group + h) * head_dim, head_dim), head_dim)] = (out / total).astype(jnp.bfloat16)

        @pl.when(s >= core_steps)
        def _():
            proj = jnp.dot(mixed[...], w_ref[...], preferred_element_type=jnp.float32).astype(jnp.bfloat16)
            for ref, start, size in zip(y_refs, starts, sizes):
                part = proj[start:start + size].astype(jnp.float32)
                out_ref[start // each, start % each:start % each + size, :] = (ref[...].astype(jnp.float32) + part).astype(jnp.bfloat16)

    core_spec = pl.BlockSpec((tokens, group * head_dim), lambda s: (0, jnp.minimum(s, core_steps - 1)))
    tail = lambda s: jnp.maximum(s - core_steps, 0)
    extra = list(deps) + ([] if previous is None else [previous])
    aliases = {} if previous is None else {4 + len(blocks) + len(deps): 0}
    return pl.pallas_call(
        body,
        out_shape=jax.ShapeDtypeStruct((micro_count, each, dim), jnp.bfloat16),
        grid=(core_steps + dim // cols,),
        in_specs=[core_spec, core_spec, core_spec, pl.BlockSpec((width, cols), lambda s: (0, tail(s)))]
        + [pl.BlockSpec((size, cols), lambda s: (0, tail(s))) for size in sizes] + [ANY] * len(extra),
        out_specs=pl.BlockSpec((micros, each, cols), lambda s: (micro // micros, 0, tail(s))),
        scratch_shapes=[pltpu.VMEM((tokens, width), jnp.bfloat16)],
        input_output_aliases=aliases,
        compiler_params=pltpu.CompilerParams(vmem_limit_bytes=VMEM_LIMIT),
        cost_estimate=pl.CostEstimate(flops=2 * tokens * width * dim, bytes_accessed=2 * width * dim, transcendentals=0),
        name="attend",
    )(queries, keys, values, w_out, *blocks, *extra)


def pick_rows(expert_out, picks, cap, deps=()):
    experts, _, dim = expert_out.shape[2:]
    step = 16
    count = len(picks)

    def body(owners_ref, *refs):
        for source_ref, out_ref in zip(refs[:count], refs[-count:]):
            out_ref[...] = source_ref[0, 0]

    def source(which, micro):
        return pl.BlockSpec((1, 1, step, cap, dim), lambda s, o: (0, micro, s, o[which], 0))

    return pl.pallas_call(
        body,
        out_shape=[jax.ShapeDtypeStruct((experts, cap, dim), expert_out.dtype)] * count,
        grid_spec=pltpu.PrefetchScalarGridSpec(
            num_scalar_prefetch=1,
            grid=(experts // step,),
            in_specs=[source(which, micro) for which, (micro, _) in enumerate(picks)] + [ANY] * len(deps),
            out_specs=[pl.BlockSpec((step, cap, dim), lambda s, o: (s, 0, 0))] * count,
        ),
        cost_estimate=pl.CostEstimate(flops=2_000_000_000 * count, bytes_accessed=4 * experts * cap * dim * count, transcendentals=0),
        name="pick",
    )(jnp.stack([owner for _, owner in picks]).astype(jnp.int32), *([expert_out] * count), *deps)


def chip_partial(expert_out, sibling_rows, micro, owner, rows, gates, tokens, top_k, chunks, deps=()):
    experts, cap, dim = sibling_rows.shape
    step = 4
    streams = 2
    tiles = dim // LANES
    steps = experts // (step * streams)
    pitch = 2 * experts * cap + 1
    count = min(128, tokens // chunks)
    while (tokens // chunks) % count:
        count -= 32
    parts = tokens // chunks // count

    def body(owner_ref, rows_ref, gates_ref, *rest):
        sources = rest[:2 * streams]
        outs, table = rest[2 * streams + len(deps):-1], rest[-1]
        s = pl.program_id(0)

        @pl.when(s < steps)
        def _():
            for k, ref in enumerate(sources):
                base = pl.multiple_of((k * steps + s) * (step * cap), 8)
                for e in range(step):
                    for j in range(tiles):
                        rows_e = ref[0, 0, e, :, j * LANES:(j + 1) * LANES] if k < streams else ref[e, :, j * LANES:(j + 1) * LANES]
                        table[pl.ds(j * pitch + base + e * cap, cap), :] = rows_e.astype(jnp.float32)

        for c, out_ref in enumerate(outs):
            first = steps + c * parts

            @pl.when((s >= first) & (s < first + parts))
            def _():
                def token(t, carry):
                    acc = None
                    for j in range(top_k):
                        at = ((s - steps) * count + t) * top_k + j
                        term = table[pl.ds(rows_ref[at], tiles, stride=pitch), :] * gates_ref[at]
                        acc = term if acc is None else acc + term
                    out_ref[pl.ds(pl.multiple_of(t * tiles, tiles), tiles), :] = acc
                    return carry

                lax.fori_loop(0, count, token, 0, unroll=8)

    def own_spec(k):
        return pl.BlockSpec((1, 1, step, cap, dim), lambda s, o, r, g: (0, micro, k * steps + jnp.minimum(s, steps - 1), o[0], 0))

    def sibling_spec(k):
        return pl.BlockSpec((step, cap, dim), lambda s, o, r, g: (k * steps + jnp.minimum(s, steps - 1), 0, 0))

    def out_spec(c):
        return pl.BlockSpec((count * tiles, LANES), lambda s, o, r, g: (jnp.clip(s - steps - c * parts, 0, parts - 1), 0))

    return pl.pallas_call(
        body,
        out_shape=[jax.ShapeDtypeStruct((parts * count * tiles, LANES), jnp.float32)] * chunks,
        grid_spec=pltpu.PrefetchScalarGridSpec(
            num_scalar_prefetch=3,
            grid=(steps + chunks * parts,),
            in_specs=[own_spec(k) for k in range(streams)] + [sibling_spec(k) for k in range(streams)] + [ANY] * len(deps),
            out_specs=[out_spec(c) for c in range(chunks)],
            scratch_shapes=[pltpu.VMEM((tiles * pitch, LANES), jnp.float32)],
        ),
        compiler_params=pltpu.CompilerParams(vmem_limit_bytes=VMEM_LIMIT),
        cost_estimate=pl.CostEstimate(flops=8_000_000_000, bytes_accessed=3 * experts * cap * dim * 2, transcendentals=0),
        name="combine",
    )(owner, rows, gates, *([expert_out] * streams), *([sibling_rows] * streams), *deps)


def combine_chunk(own_part, far_part, residual, shared, start, sh_start, deps=()):
    dim = residual.shape[1]
    tiles = dim // LANES
    chunk = own_part.shape[0] // tiles
    block = 96 if chunk % 96 == 0 else ROWS
    pitch = block + 2

    def body(own_ref, far_ref, res_ref, sh_ref, *rest):
        out_ref, planes = rest[-2:]

        def token(t, carry):
            at = pl.ds(pl.multiple_of(t * tiles, tiles), tiles)
            planes[pl.ds(t, tiles, stride=pitch), :] = own_ref[at, :] + far_ref[at, :]
            return carry

        lax.fori_loop(0, block, token, 0, unroll=8)
        for j in range(tiles):
            at = slice(j * LANES, (j + 1) * LANES)
            total = res_ref[:, at].astype(jnp.float32) + sh_ref[:, at].astype(jnp.float32) + planes[j * pitch:j * pitch + block, :]
            out_ref[:, at] = total.astype(jnp.bfloat16)

    part_spec = pl.BlockSpec((block * tiles, LANES), lambda s: (s, 0))
    rows_from = lambda first: pl.BlockSpec((block, dim), lambda s: (first // block + s, 0))
    return pl.pallas_call(
        body,
        out_shape=jax.ShapeDtypeStruct((chunk, dim), jnp.bfloat16),
        grid=(chunk // block,),
        in_specs=[part_spec, part_spec, rows_from(start), rows_from(sh_start)] + [ANY] * len(deps),
        out_specs=pl.BlockSpec((block, dim), lambda s: (s, 0)),
        scratch_shapes=[pltpu.VMEM((tiles * pitch, LANES), jnp.float32)],
        cost_estimate=pl.CostEstimate(flops=1_000_000_000, bytes_accessed=14 * chunk * dim, transcendentals=0),
        name="finish",
    )(own_part, far_part, residual, shared, *deps)


def solution(mesh):
    stages = mesh.shape["pp"]
    ep_size = mesh.shape["ep"]
    shift_pairs = [(source, (source + 1) % stages) for source in range(stages)]
    core_pairs = [(source, source ^ 1) for source in range(ep_size)]
    chip_pairs = [(source, (source + 2) % ep_size) for source in range(ep_size)]
    tok_spec = P("pp", "data", "ep", None, None)
    vec_spec = P("pp", None)
    mat_spec = P("pp", None, None)
    head_spec = P("pp", None, None, None)

    def device_step(expert_out, expert_ids, slot_ids, gate_weights, residual, norm_moe, w_gate, w_up, w_down, norm_attn, w_query, w_key, w_value, w_out):
        micro_count, local_experts, slots_total, dim = expert_out.shape[1:]
        seqs, seq_len, top_k = expert_ids.shape[2:]
        tokens = seqs * seq_len
        cap = slots_total // ep_size
        me = lax.axis_index("ep")
        chip, core = me // 2, me % 2
        far = (me + 2) % ep_size
        as_owner = lambda who: jnp.reshape(who, (1,)).astype(jnp.int32)

        home = expert_ids[0] // local_experts
        slot = slot_ids[0]
        row_here = (expert_ids[0] % local_experts) * cap + (slot - me * cap)

        def routing(on_chip):
            usable = (slot >= 0) & (home // 2 == on_chip)
            row = row_here + jnp.where(home % 2 == core, 0, local_experts * cap)
            flat = (micro_count, tokens * top_k)
            return jnp.where(usable, row, 0).reshape(flat), jnp.where(usable, gate_weights[0], 0.0).reshape(flat)

        own_rows, own_gates = routing(chip)
        send_rows, send_gates = routing(1 - chip)
        far_meta = lax.ppermute(jnp.stack([send_rows.astype(jnp.float32), send_gates]), "ep", chip_pairs)
        far_rows, far_gates = far_meta[0].astype(jnp.int32), far_meta[1]

        to_far = lambda m: (m, far ^ 1)
        to_own = lambda m: (m, me ^ 1)
        pick_plan = ([to_far(0)], [to_far(1)], [to_far(2), to_own(0)], [to_far(3), to_own(1)], [to_own(2), to_own(3)])
        from_sibling = []

        def exchange(step, deps):
            picked = pick_rows(expert_out, pick_plan[step], cap, deps)
            from_sibling.append([lax.ppermute(rows, "ep", core_pairs) for rows in picked])
            return (picked[-1],)

        last = exchange(1, exchange(0, ()))
        arrived = []
        for m in range(micro_count):
            parts = chip_partial(expert_out, from_sibling[m][0], m, as_owner(far), far_rows[m], far_gates[m], tokens, top_k, CHUNKS[m], last)
            last = (parts[0],)
            arrived.append([])
            for part in parts:
                arrived[m].append(lax.ppermute(part, "ep", chip_pairs))
            if m + 2 < len(pick_plan):
                last = exchange(m + 2, last)
        own_sib = [from_sibling[2][1], from_sibling[3][1], *from_sibling[4]]

        flat_resid = residual.reshape(micro_count * tokens, dim)
        heads_width = w_query.shape[2] * w_query.shape[3]
        flat = lambda weight: weight[0].reshape(dim, heads_width)

        def own(m, deps):
            return chip_partial(expert_out, own_sib[m], m, as_owner(me), own_rows[m], own_gates[m], tokens, top_k, CHUNKS[m], deps)

        halves = 2
        half_tokens = micro_count * tokens // halves
        hidden_half = lambda part, deps: gated_hidden(flat_resid, part, halves, norm_moe, w_gate[0], w_up[0], deps)
        shared = [down_product(hidden_half(0, last), w_down[0])]
        here = [None] * micro_count
        pieces = [[] for _ in range(micro_count)]

        def finish(m, c, deps):
            chunk = tokens // CHUNKS[m]
            start = m * tokens + c * chunk
            combined = combine_chunk(here[m][c], arrived[m][c], flat_resid, shared[start // half_tokens], start, start % half_tokens, deps)
            pieces[m].append(lax.ppermute(combined, "pp", shift_pairs))
            return (combined,)

        def project(micros, deps):
            normed = normalize([piece for m in micros for piece in pieces[m]], norm_attn, deps)
            return [jnp.dot(normed, flat(weight), preferred_element_type=jnp.float32).astype(jnp.bfloat16) for weight in (w_query, w_key, w_value)]

        def mix(micros, projected, previous, deps):
            blocks = [piece for m in micros for piece in pieces[m]]
            return attend(*projected, blocks, w_out[0].reshape(heads_width, dim), micros[0], tokens, micro_count, seq_len, w_query.shape[3], previous, deps)

        here[0] = own(0, (shared[0],))
        last = finish(0, 0, (here[0][0],))
        hidden = hidden_half(1, last)
        here[1] = own(1, (hidden,))
        last = finish(1, 1, finish(1, 0, (here[1][0],)))
        shared.append(down_product(hidden, w_down[0], last))
        here[2] = own(2, (shared[1],))
        last = finish(1, 2, (here[2][0],))
        here[3] = own(3, last)
        both = project((0, 1), (here[3][0],))
        last = finish(2, 0, (both[2],))
        last = finish(2, 1, (*both, *last))
        out = mix((0, 1), both, None, last)
        last = finish(3, 0, (out,))
        third = project((2,), last)
        last = finish(3, 1, (third[2],))
        last = finish(3, 2, (third[1], *last))
        out = mix((2,), third, out, last)
        fourth = project((3,), (out,))
        out = mix((3,), fourth, out, ())
        return out.reshape(residual.shape)

    in_specs = (tok_spec,) * 5 + (vec_spec, mat_spec, mat_spec, mat_spec, vec_spec, head_spec, head_spec, head_spec, head_spec)

    return jax.shard_map(device_step, mesh=mesh, in_specs=in_specs, out_specs=tok_spec, check_vma=False)
```
